32 devices in a mesh: dp: 4 (over y, z), sp: 8 (over x, core).
Axes of the slice: x: 4, y: 2, z: 2, core: 2. Of those that a mesh axis runs over, the one named last changes fastest.
The devices are a block of a 4x4x8 slice.
Arguments:
- x: bfloat16 [4, 6144, 2560], P('dp', 'sp'), parts along dimension 0
- segment_ids: int32 [4, 6144], P('dp', 'sp'), parts along dimension 0
- positions: int32 [4, 6144], P('dp', 'sp'), parts along dimension 0
- out_grad: bfloat16 [4, 6144, 2560], P('dp', 'sp'), parts along dimension 0
- norm_scale: bfloat16 [2560], replicated
- w_q: bfloat16 [2560, 2048], replicated
- w_k: bfloat16 [2560, 256], replicated
- w_v: bfloat16 [2560, 256], replicated
- w_o: bfloat16 [2048, 2560], replicated
- b_o: bfloat16 [2560], replicated
Outputs:
- output 1: bfloat16 [4, 6144, 2560], P('dp', 'sp'), parts along dimension 0
- output 2: bfloat16 [4, 6144, 2560], P('dp', 'sp'), parts along dimension 0
- output 3: bfloat16 [10240], P('dp'), parts along dimension 0
- output 4: bfloat16 [10240, 2048], P('dp'), parts along dimension 0
- output 5: bfloat16 [10240, 256], P('dp'), parts along dimension 0
- output 6: bfloat16 [10240, 256], P('dp'), parts along dimension 0
- output 7: bfloat16 [8192, 2560], P('dp'), parts along dimension 0
- output 8: bfloat16 [10240], P('dp'), parts along dimension 0
There are 4 independent parts. The reference program is written for one: setup_inputs(seed, part) draws one part's arguments, and reference() takes and returns one part's arrays. A program takes and returns all parts, laid end to end along the dimension named above; an argument that names none is the same for every part.
All inputs are finite; a program needn't handle non-finite values.
Results may differ from the reference program's by a relative error of at most 0.0180483.
Values are sent between devices in bfloat16 or wider.
A program may use at most 768 MiB of HBM per device.

```python
import jax
import jax.numpy as jnp
from jax import lax

BATCH_SIZE = 1
SEQ_LEN = 6144
MODEL_DIM = 2560
NUM_HEADS = 8
HEAD_DIM = 256
WINDOW = 2048
QUERY_BLOCK = 128
DOC_MEAN = max(QUERY_BLOCK, min(2 * WINDOW, SEQ_LEN // 4))
QK_GAIN = 1.7
NORM_EPS = 1e-6
ROPE_BASE = 10000.0
NEG_BIG = -1e30


def draw_documents(start_key, offset_key):
    token_idx = jnp.arange(SEQ_LEN, dtype=jnp.int32)[None, :]
    starts = jax.random.randint(start_key, (BATCH_SIZE, SEQ_LEN), 0, DOC_MEAN) == 0
    starts = starts & (token_idx > 0)
    seg_ids = jnp.cumsum(starts.astype(jnp.int32), axis=1).astype(jnp.int32)
    doc_start = lax.cummax(jnp.where(starts, token_idx, 0), axis=1)
    row_offset = jax.random.randint(offset_key, (BATCH_SIZE, 1), 0, 4096)
    positions = (token_idx - doc_start + row_offset).astype(jnp.int32)
    return seg_ids, positions


def setup_inputs(seed: int = 0, part: int = 0) -> dict:
    shared_keys = jax.random.split(jax.random.key(seed), 7)
    part_keys = jax.random.split(jax.random.fold_in(jax.random.key(seed + 1), part), 4)
    seg_ids, positions = draw_documents(part_keys[2], part_keys[3])
    act_shape = (BATCH_SIZE, SEQ_LEN, MODEL_DIM)
    q_width = NUM_HEADS * HEAD_DIM
    in_std = MODEL_DIM ** -0.5

    def normal_bf16(rng_key, shape, std_dev):
        return (jax.random.normal(rng_key, shape, jnp.float32) * std_dev).astype(jnp.bfloat16)

    return {
        "x": normal_bf16(part_keys[0], act_shape, 1.0),
        "segment_ids": seg_ids,
        "positions": positions,
        "out_grad": normal_bf16(part_keys[1], act_shape, 1.0),
        "norm_scale": normal_bf16(shared_keys[0], (MODEL_DIM,), 0.3),
        "w_q": normal_bf16(shared_keys[1], (MODEL_DIM, q_width), QK_GAIN * in_std),
        "w_k": normal_bf16(shared_keys[2], (MODEL_DIM, HEAD_DIM), QK_GAIN * in_std),
        "w_v": normal_bf16(shared_keys[3], (MODEL_DIM, HEAD_DIM), in_std),
        "w_o": normal_bf16(shared_keys[4], (q_width, MODEL_DIM), q_width ** -0.5),
        "b_o": normal_bf16(shared_keys[5], (MODEL_DIM,), 0.3),
    }


def rms_norm(x_f32, norm_gain):
    mean_sq = jnp.mean(x_f32 * x_f32, axis=-1, keepdims=True)
    return (x_f32 * lax.rsqrt(mean_sq + NORM_EPS) * (1.0 + norm_gain.astype(jnp.float32))).astype(jnp.bfloat16)


def rotary(head_vals, positions):
    rot_dim = HEAD_DIM // 2
    half_dim = rot_dim // 2
    inv_freq = ROPE_BASE ** (-(jnp.arange(half_dim, dtype=jnp.float32) * 2.0 / rot_dim))
    angles = positions.astype(jnp.float32)[:, :, None, None] * inv_freq
    cos_a = jnp.cos(angles)
    sin_a = jnp.sin(angles)
    first_half = head_vals[..., :half_dim]
    second_half = head_vals[..., half_dim:rot_dim]
    return jnp.concatenate([first_half * cos_a - second_half * sin_a, second_half * cos_a + first_half * sin_a, head_vals[..., rot_dim:]], axis=-1)


def attention(queries, keys_in, values_in, seg_ids):
    batch_rows, seq_len, n_heads, head_dim = queries.shape
    key_span = WINDOW + QUERY_BLOCK
    keys_pad = jnp.pad(keys_in, ((0, 0), (WINDOW, 0), (0, 0)))
    values_pad = jnp.pad(values_in, ((0, 0), (WINDOW, 0), (0, 0)))
    seg_pad = jnp.pad(seg_ids, ((0, 0), (WINDOW, 0)), constant_values=-1)
    offsets = jnp.arange(key_span)[None, :]
    row_idx = jnp.arange(QUERY_BLOCK)[:, None]
    in_band = (offsets > row_idx) & (offsets <= row_idx + WINDOW)

    def one_block(q_start):
        q_blk = lax.dynamic_slice_in_dim(queries, q_start, QUERY_BLOCK, axis=1)
        k_blk = lax.dynamic_slice_in_dim(keys_pad, q_start, key_span, axis=1)
        v_blk = lax.dynamic_slice_in_dim(values_pad, q_start, key_span, axis=1)
        q_seg = lax.dynamic_slice_in_dim(seg_ids, q_start, QUERY_BLOCK, axis=1)
        k_seg = lax.dynamic_slice_in_dim(seg_pad, q_start, key_span, axis=1)
        allowed = (q_seg[:, :, None] == k_seg[:, None, :]) & in_band[None]
        scores = jnp.einsum("bqhe,bke->bhqk", q_blk.astype(jnp.float32), k_blk.astype(jnp.float32))
        scores = jnp.where(allowed[:, None], scores, NEG_BIG)
        attn_prob = jax.nn.softmax(scores, axis=-1).astype(jnp.bfloat16)
        o_blk = jnp.einsum("bhqk,bke->bqhe", attn_prob.astype(jnp.float32), v_blk.astype(jnp.float32))
        return o_blk.astype(jnp.bfloat16)

    blocks = lax.map(jax.checkpoint(one_block), jnp.arange(seq_len // QUERY_BLOCK) * QUERY_BLOCK)
    return jnp.moveaxis(blocks, 0, 1).reshape(batch_rows, seq_len, n_heads, head_dim)


def forward(x, norm_scale, w_q, w_k, w_v, w_o, b_o, seg_ids, positions):
    x_f32 = x.astype(jnp.float32)
    normed = rms_norm(x_f32, norm_scale)
    q_lin = jnp.dot(normed, w_q, preferred_element_type=jnp.float32).reshape(BATCH_SIZE, SEQ_LEN, NUM_HEADS, HEAD_DIM)
    queries = (rotary(q_lin, positions) * HEAD_DIM ** -0.5).astype(jnp.bfloat16)
    keys_all = rotary(jnp.dot(normed, w_k, preferred_element_type=jnp.float32)[:, :, None, :], positions)[:, :, 0, :].astype(jnp.bfloat16)
    values_all = jnp.dot(normed, w_v, preferred_element_type=jnp.float32).astype(jnp.bfloat16)
    attn_out = attention(queries, keys_all, values_all, seg_ids)
    y_proj = jnp.dot(attn_out.reshape(BATCH_SIZE, SEQ_LEN, NUM_HEADS * HEAD_DIM), w_o, preferred_element_type=jnp.float32)
    return (x_f32 + y_proj + b_o.astype(jnp.float32)).astype(jnp.bfloat16)


def reference(x, segment_ids, positions, out_grad, norm_scale, w_q, w_k, w_v, w_o, b_o):
    def block_fn(x_in, gain_in, wq_in, wk_in, wv_in, wo_in, bo_in):
        return forward(x_in, gain_in, wq_in, wk_in, wv_in, wo_in, bo_in, segment_ids, positions)

    block_out, pull_back = jax.vjp(block_fn, x, norm_scale, w_q, w_k, w_v, w_o, b_o)
    all_grads = pull_back(out_grad)
    return (block_out, all_grads[0], all_grads[1], all_grads[2], all_grads[3], all_grads[4], all_grads[5], all_grads[6])
```

```python
import functools

import jax
import jax.numpy as jnp
from jax import lax
from jax.experimental import pallas as pl
from jax.experimental.pallas import tpu as pltpu
from jax.sharding import PartitionSpec as P

WINDOW = 2048
NORM_EPS = 1e-6
ROPE_BASE = 10000.0
NEG_BIG = -1e30
QB = 256
CHUNKS = 3
HEAD_GROUPS = 2


def rms_norm(x_f32, gain_f32):
    mean_sq = jnp.mean(x_f32 * x_f32, axis=-1, keepdims=True)
    return (x_f32 * lax.rsqrt(mean_sq + NORM_EPS) * (1.0 + gain_f32)).astype(jnp.bfloat16)


def nt(a, b):
    return lax.dot_general(a, b, (((1,), (1,)), ((), ())), preferred_element_type=jnp.float32)


def nn(a, b):
    return jnp.dot(a, b, preferred_element_type=jnp.float32)


def attend(q_ref, dot_ref, k_ref, v_ref, kt_ref, vt_ref, lo_ref, s_ref, pb_ref, ot_ref, dqt_ref, dk_ref, dv_ref):
    span = WINDOW + QB
    ch = span // CHUNKS

    def block(qb, carry):
        r0 = pl.multiple_of(qb * QB, QB)
        q_b = q_ref[pl.ds(r0, QB), :]
        dot_b = dot_ref[:, pl.ds(r0, QB)]
        lo = lo_ref[:, pl.ds(r0, QB)]
        m = None
        for c in range(CHUNKS):
            s = nt(k_ref[pl.ds(pl.multiple_of(r0 + c * ch, QB), ch), :], q_b)
            row = lax.broadcasted_iota(jnp.int32, (ch, QB), 0) + c * ch
            ok = row >= lo - r0
            if (c + 1) * ch > WINDOW:
                ok = ok & (row - WINDOW <= lax.broadcasted_iota(jnp.int32, (ch, QB), 1))
            s = jnp.where(ok, s, NEG_BIG)
            s_ref[pl.ds(c * ch, ch), :] = s
            mc = jnp.max(s, axis=0, keepdims=True)
            m = mc if m is None else jnp.maximum(m, mc)
        total = None
        for c in range(CHUNKS):
            p = jnp.exp(s_ref[pl.ds(c * ch, ch), :] - m)
            s_ref[pl.ds(c * ch, ch), :] = p
            t = jnp.sum(p, axis=0, keepdims=True)
            total = t if total is None else total + t
        inv = 1.0 / total
        for c in range(CHUNKS):
            p = s_ref[pl.ds(c * ch, ch), :] * inv
            pb = p.astype(jnp.bfloat16)
            pb_ref[pl.ds(c * ch, ch), :] = pb
            rows = pl.ds(pl.multiple_of(r0 + c * ch, QB), ch)
            dv_ref[rows, :] += nt(pb, dot_b)
        o_t = nn(vt_ref[:, pl.ds(r0, span)], pb_ref[...])
        ot_ref[:, pl.ds(r0, QB)] = o_t.astype(jnp.bfloat16)
        delta = jnp.sum(o_t * dot_b.astype(jnp.float32), axis=0, keepdims=True)
        for c in range(CHUNKS):
            rows = pl.ds(pl.multiple_of(r0 + c * ch, QB), ch)
            dp = nn(v_ref[rows, :], dot_b)
            ds = (s_ref[pl.ds(c * ch, ch), :] * inv * (dp - delta)).astype(jnp.bfloat16)
            pb_ref[pl.ds(c * ch, ch), :] = ds
            dk_ref[rows, :] += nn(ds, q_b)
        dqt_ref[:, pl.ds(r0, QB)] = nn(kt_ref[:, pl.ds(r0, span)], pb_ref[...])
        return carry

    lax.fori_loop(0, q_ref.shape[0] // QB, block, 0)


def heads_kernel(n_ref, og_ref, k_ref, v_ref, kt_ref, vt_ref, lo_ref, cos_ref, sin_ref, cost_ref, sint_ref, wq_ref, wo_ref,
                 ot_ref, dql_ref, g_ref, dk_ref, dv_ref, q_ref, dot_ref, s_ref, pb_ref, dqt_ref):
    e = wq_ref.shape[1]
    half = e // 2
    quarter = e // 4

    @pl.when(pl.program_id(0) == 0)
    def _():
        dk_ref[...] = jnp.zeros_like(dk_ref)
        dv_ref[...] = jnp.zeros_like(dv_ref)

    q_lin = nn(n_ref[...], wq_ref[...])
    rot = q_lin[:, :half]
    rot = rot * cos_ref[...] + pltpu.roll(rot, quarter, 1) * sin_ref[...]
    scale = e ** -0.5
    q_ref[:, :half] = (rot * scale).astype(jnp.bfloat16)
    q_ref[:, half:] = (q_lin[:, half:] * scale).astype(jnp.bfloat16)
    dot_ref[...] = nt(wo_ref[...], og_ref[...]).astype(jnp.bfloat16)
    attend(q_ref, dot_ref, k_ref, v_ref, kt_ref, vt_ref, lo_ref, s_ref, pb_ref, ot_ref, dqt_ref, dk_ref, dv_ref)
    dq = dqt_ref[...].astype(jnp.bfloat16).astype(jnp.float32)
    a, b = dq[:quarter], dq[quarter:half]
    ct, st = cost_ref[...], sint_ref[...]
    dql_ref[:quarter] = ((a * ct + b * st) * scale).astype(jnp.bfloat16)
    dql_ref[quarter:half] = ((b * ct - a * st) * scale).astype(jnp.bfloat16)
    dql_ref[half:] = (dq[half:] * scale).astype(jnp.bfloat16)
    g_ref[:e] = nn(dql_ref[...], n_ref[...])
    g_ref[e:] = nn(ot_ref[...], og_ref[...])


def run_heads(first, count, e, normed, out_grad, keys, values, keys_t, values_t, lo, cos2, sin2, cos_t, sin_t, w_q, w_o):
    tok, d = normed.shape
    span = keys.shape[0]
    full = pl.BlockSpec(memory_space=pltpu.VMEM)
    head_cols = pl.BlockSpec((d, e), lambda h: (0, h + first))
    head_rows = pl.BlockSpec((e, d), lambda h: (h + first, 0))
    flops = count * (2 * tok * e * (WINDOW + QB) * 6 + 8 * tok * d * e)
    return pl.pallas_call(
        heads_kernel,
        grid=(count,),
        in_specs=[full] * 11 + [head_cols, head_rows],
        out_specs=[
            pl.BlockSpec((e, tok), lambda h: (h, 0)),
            pl.BlockSpec((e, tok), lambda h: (h, 0)),
            pl.BlockSpec((2 * e, d), lambda h: (h, 0)),
            pl.BlockSpec((span, e), lambda h: (0, 0)),
            pl.BlockSpec((span, e), lambda h: (0, 0)),
        ],
        out_shape=[
            jax.ShapeDtypeStruct((count * e, tok), jnp.bfloat16),
            jax.ShapeDtypeStruct((count * e, tok), jnp.bfloat16),
            jax.ShapeDtypeStruct((count * 2 * e, d), jnp.float32),
            jax.ShapeDtypeStruct((span, e), jnp.float32),
            jax.ShapeDtypeStruct((span, e), jnp.float32),
        ],
        scratch_shapes=[
            pltpu.VMEM((tok, e), jnp.bfloat16),
            pltpu.VMEM((e, tok), jnp.bfloat16),
            pltpu.VMEM((WINDOW + QB, QB), jnp.float32),
            pltpu.VMEM((WINDOW + QB, QB), jnp.bfloat16),
            pltpu.VMEM((e, tok), jnp.float32),
        ],
        compiler_params=pltpu.CompilerParams(dimension_semantics=("arbitrary",), vmem_limit_bytes=62 * 1024 * 1024),
        cost_estimate=pl.CostEstimate(flops=flops, bytes_accessed=40 * 2 ** 20, transcendentals=0),
        name="heads",
    )(normed, out_grad, keys, values, keys_t, values_t, lo, cos2, sin2, cos_t, sin_t, w_q, w_o)


def solution(mesh):
    row_spec = P("dp", "sp", None)
    tok_spec = P("dp", "sp")
    mat_spec = P(None, None)
    grad_mat = P("dp", None)
    n_sp = mesh.shape["sp"]

    def shift(val, k):
        return lax.ppermute(val, "sp", [(i, i + k) for i in range(n_sp - k)])

    def unshift(val, k):
        return lax.ppermute(val, "sp", [(i, i - k) for i in range(k, n_sp)])

    def local_step(x, seg_ids, positions, out_grad, norm_scale, w_q, w_k, w_v, w_o, b_o):
        x, seg, pos, og = x[0], seg_ids[0], positions[0], out_grad[0]
        tok = x.shape[0]
        e = w_k.shape[1]
        n_heads = w_q.shape[1] // e
        me = lax.axis_index("sp")
        halo = -(-WINDOW // tok)
        sizes = [min(tok, WINDOW - (k - 1) * tok) for k in range(1, halo + 1)]

        seg_parts = [jnp.where(me >= k, shift(seg[tok - size:], k), -1) for k, size in zip(range(1, halo + 1), sizes)]
        seg_k = jnp.concatenate(seg_parts[::-1] + [seg])
        lo_doc = jnp.sum((seg_k[None, :] < seg[:, None]).astype(jnp.int32), axis=1)
        lo = jnp.maximum(lo_doc, jnp.arange(tok, dtype=jnp.int32) + 1)[None, :]

        quarter = e // 4
        inv_freq = ROPE_BASE ** (-(jnp.arange(quarter, dtype=jnp.float32) * 4.0 / e))
        angles = pos.astype(jnp.float32)[:, None] * inv_freq
        cos_a, sin_a = jnp.cos(angles), jnp.sin(angles)
        cos2 = jnp.concatenate([cos_a, cos_a], axis=1)
        sin2 = jnp.concatenate([-sin_a, sin_a], axis=1)

        def rotate(vals, sign):
            a, b = vals[:, :quarter], vals[:, quarter:2 * quarter]
            return jnp.concatenate([a * cos_a - sign * b * sin_a, b * cos_a + sign * a * sin_a, vals[:, 2 * quarter:]], axis=1)

        x_f32 = x.astype(jnp.float32)
        normed, norm_pull = jax.vjp(rms_norm, x_f32, norm_scale.astype(jnp.float32))
        k_loc = rotate(nn(normed, w_k), 1.0).astype(jnp.bfloat16)
        v_loc = nn(normed, w_v).astype(jnp.bfloat16)
        kv = jnp.concatenate([k_loc, v_loc], axis=1)
        kv_all = jnp.concatenate([shift(kv[tok - size:], k) for k, size in zip(range(1, halo + 1), sizes)][::-1] + [kv], axis=0)
        keys, values = kv_all[:, :e], kv_all[:, e:]
        keys_t, values_t = keys.T, values.T

        per = n_heads // HEAD_GROUPS
        o_parts, dq_parts, grads, dkv = [], [], [], 0.0
        for g in range(HEAD_GROUPS):
            o_t, dq_t, part, dk, dv = run_heads(g * per, per, e, normed, og, keys, values, keys_t, values_t, lo, cos2, sin2, cos_a.T, sin_a.T, w_q, w_o)
            o_parts.append(o_t)
            dq_parts.append(dq_t)
            mine = lax.psum_scatter(part, "sp", scatter_dimension=0, tiled=True).astype(jnp.bfloat16)
            grads.append(lax.all_gather(mine, "sp", axis=0, tiled=True).reshape(per, 2, e, -1))
            dkv = dkv + jnp.concatenate([dk, dv], axis=1)

        own = dkv[WINDOW:]
        start = WINDOW
        for k, size in zip(range(1, halo + 1), sizes):
            start -= size
            own = own + jnp.pad(unshift(dkv[start:start + size], k), ((tok - size, 0), (0, 0)))
        dk_lin = rotate(own[:, :e].astype(jnp.bfloat16).astype(jnp.float32), -1.0).astype(jnp.bfloat16)
        dv_lin = own[:, e:].astype(jnp.bfloat16)
        dkv_lin = jnp.concatenate([dk_lin, dv_lin], axis=1)
        kv_part = lax.dot_general(dkv_lin, normed, (((0,), (0,)), ((), ())), preferred_element_type=jnp.float32)
        kv_mine = lax.psum_scatter(kv_part, "sp", scatter_dimension=0, tiled=True).astype(jnp.bfloat16)
        kv_grad = lax.all_gather(kv_mine, "sp", axis=0, tiled=True)

        o_t = jnp.concatenate(o_parts, axis=0)
        dq_t = jnp.concatenate(dq_parts, axis=0)
        y = lax.dot_general(o_t, w_o, (((0,), (0,)), ((), ())), preferred_element_type=jnp.float32)
        block_out = (x_f32 + y + b_o.astype(jnp.float32)).astype(jnp.bfloat16)
        d_normed = (lax.dot_general(dq_t, w_q, (((0,), (1,)), ((), ())), preferred_element_type=jnp.float32)
                    + nt(dk_lin, w_k) + nt(dv_lin, w_v)).astype(jnp.bfloat16)
        dx_norm, gain_part = norm_pull(d_normed)
        x_grad = (og.astype(jnp.float32) + dx_norm).astype(jnp.bfloat16)
        b_part = jnp.sum(og, axis=0, dtype=jnp.float32)
        small = lax.psum(jnp.stack([gain_part, b_part]), "sp").astype(jnp.bfloat16)
        w_q_grad = jnp.concatenate([g[:, 0].reshape(per * e, -1) for g in grads], axis=0).T
        w_o_grad = jnp.concatenate([g[:, 1].reshape(per * e, -1) for g in grads], axis=0)
        return (block_out[None], x_grad[None], small[0], w_q_grad, kv_grad[:e].T, kv_grad[e:].T, w_o_grad, small[1])

    return jax.shard_map(local_step, mesh=mesh,
                         in_specs=(row_spec, tok_spec, tok_spec, row_spec, P(None), mat_spec, mat_spec, mat_spec, mat_spec, P(None)),
                         out_specs=(row_spec, row_spec, P("dp"), grad_mat, grad_mat, grad_mat, grad_mat, P("dp")),
                         check_vma=False)
```
